32 devices in a mesh: seq: 8 (over y, x, core), head: 4 (over z).
Axes of the slice: x: 2, y: 2, z: 4, core: 2. Of those that a mesh axis runs over, the one named last changes fastest.
Arguments:
- key_rows: bfloat16 [2048, 2048], P('seq', 'head'), may hold values from -1 to 1, as said below
- values: bfloat16 [2048, 2048], P('seq', 'head'), may hold values from -6 to 6
- d_layer: bfloat16 [2048, 2048], P('seq', 'head'), may hold values from -6 to 6
- out_weight: bfloat16 [2048, 2048], P('head'), may hold values from -0.125 to 0.125
- saved_solutions: float32 [2048, 2048], P('seq', 'head'), may hold values from -0.625 to 0.625
- ridge_scale: float32 [16], P('head'), may hold values from 0.5 to 4
Outputs:
- grad_queries: float32 [2048, 2048], P('seq', 'head')
- grad_keys: float32 [2048, 2048], P('seq', 'head')
- grad_values: float32 [2048, 2048], P('seq', 'head')
The draws below stay inside these ranges and needn't reach their ends.
Inputs may be any that keep to these rules, and one draw needn't show every extreme that they name: `key_rows`: within each head the 128 entries of a key have Euclidean norm 1 up to bfloat16 rounding.
All inputs are finite; a program needn't handle non-finite values.
Results may differ from the reference program's by a relative error of at most 0.0029.
Values may be sent and summed in bfloat16 or wider, within the bound.
A program may use at most 64 MiB of HBM per device.

```python
import math
import jax
import jax.numpy as jnp
from jax import lax

DM = 2048
HEADS = 16
DH = 128
TOK_DEV = 256
ITERS = 8
WIN = 512
TOKENS = 2048


def draw_key_rows(key, part):
    scale_key = jax.random.fold_in(key, 11)
    entry_key = jax.random.fold_in(key, 23)
    channel_scales = jnp.exp(jax.random.uniform(scale_key, (HEADS * DH,), jnp.float32, jnp.log(0.3), jnp.log(1.5)))
    entries = jnp.clip(jax.random.normal(entry_key, (TOKENS, HEADS * DH), jnp.float32), -6.0, 6.0)
    scaled = (entries * channel_scales).reshape(TOKENS, HEADS, DH)
    lengths = jnp.sqrt(jnp.sum(scaled * scaled, axis=-1, keepdims=True) + 1e-06)
    return (scaled / lengths).reshape(TOKENS, HEADS * DH).astype(jnp.bfloat16)


def levels(stream_key, extent, cuts, least, largest):
    level, own = 1.0, jax.random.fold_in(stream_key, 6)
    for axis_at, parts in cuts:
        steps = jnp.exp(jax.random.uniform(jax.random.fold_in(own, axis_at), (parts,), jnp.float32, least / len(cuts), largest / len(cuts)))
        level = level * jnp.repeat(steps, extent[axis_at] // parts).reshape([-1 if axis == axis_at else 1 for axis in range(len(extent))])
    return level


def normal_values(stream_key, extent, spread, bound, pieces=(), kind=jnp.bfloat16):
    factor_of = levels(stream_key, extent, pieces, -0.22, 0.18) if pieces else 1.0
    values = jax.random.normal(stream_key, extent, jnp.float32) * spread * factor_of
    return jnp.minimum(jnp.maximum(values, -bound), bound).astype(kind)


def setup_inputs(seed: int = 0) -> dict:
    arg_keys = jax.random.split(jax.random.key(seed), 7)
    key_rows = draw_key_rows(jax.random.fold_in(arg_keys[6], 71), 0)
    values = normal_values(arg_keys[1], (TOKENS, HEADS * DH), 1.0, 6.0, ((0, 8), (1, 4)))
    d_layer = normal_values(arg_keys[2], (TOKENS, DM), 1.0, 6.0, ((0, 8), (1, 4)))
    out_weight = normal_values(arg_keys[3], (HEADS * DH, DM), DM ** -0.5, 0.125, ((0, 4),))
    saved_solutions = normal_values(arg_keys[4], (TOKENS, HEADS * DH), (WIN ** -0.5), 0.625, ((0, 8), (1, 4)), jnp.float32)
    ridge_scale = jnp.clip(jnp.exp(math.log(4.0) - 2.0794415 * jax.random.uniform(arg_keys[5], (HEADS,), jnp.float32) ** levels(arg_keys[5], (HEADS,), ((0, 4),), -0.2, 0.2)), 0.5, 4.0)
    return dict(key_rows=key_rows, values=values, d_layer=d_layer, out_weight=out_weight, saved_solutions=saved_solutions, ridge_scale=ridge_scale)


HIGHEST_PRECISION = lax.Precision.HIGHEST
EPSILON = 1e-6


def make_lower(block_len):
    row_ids = lax.broadcasted_iota(jnp.int32, (block_len, block_len), 0)
    col_ids = lax.broadcasted_iota(jnp.int32, (block_len, block_len), 1)
    return (row_ids >= col_ids).astype(jnp.float32)


def shift_down(blocks, amount):
    padding = jnp.zeros((amount,) + blocks.shape[1:], blocks.dtype)
    return jnp.concatenate([padding, blocks[: blocks.shape[0] - amount]], axis=0)


def shift_up(blocks, amount):
    padding = jnp.zeros((amount,) + blocks.shape[1:], blocks.dtype)
    return jnp.concatenate([blocks[amount:], padding], axis=0)


def masked_apply(left, right, carried, mask_table):
    scores = jnp.einsum("bid,bjd->bij", left, right, precision=HIGHEST_PRECISION) * mask_table
    return jnp.einsum("bij,bjd->bid", scores, carried, precision=HIGHEST_PRECISION)


def outer_sums(left, right):
    return jnp.einsum("bid,bie->bde", left, right, precision=HIGHEST_PRECISION)


def one_head(operands):
    key_part, value_part, saved_part, dout_part, ridge_value = operands
    block_len = min(512, TOK_DEV)
    block_count = TOKENS // block_len
    lag_blocks = WIN // block_len
    key_blk = key_part.reshape(block_count, block_len, DH)
    val_blk = value_part.reshape(block_count, block_len, DH)
    sav_blk = saved_part.reshape(block_count, block_len, DH)
    out_blk = dout_part.reshape(block_count, block_len, DH)
    lower_table = make_lower(block_len)
    upper_table = lower_table.T

    gram_blocks = outer_sums(key_blk, key_blk)
    state_blocks = outer_sums(val_blk, key_blk)
    gram_before = jnp.cumsum(gram_blocks, axis=0) - gram_blocks
    state_before = jnp.cumsum(state_blocks, axis=0) - state_blocks
    gram_base = gram_before - shift_down(gram_before, lag_blocks)
    state_base = state_before - shift_down(state_before, lag_blocks)
    key_lag = shift_down(key_blk, lag_blocks)
    val_lag = shift_down(val_blk, lag_blocks)

    adjoint_rhs = jnp.einsum("bif,bfe->bie", out_blk, state_base, precision=HIGHEST_PRECISION)
    adjoint_rhs = adjoint_rhs + masked_apply(out_blk, val_blk, key_blk, lower_table)
    adjoint_rhs = adjoint_rhs - masked_apply(out_blk, val_lag, key_lag, lower_table)

    def apply_gram(vectors):
        result = jnp.einsum("bid,bde->bie", vectors, gram_base, precision=HIGHEST_PRECISION)
        result = result + masked_apply(vectors, key_blk, key_blk, lower_table)
        result = result - masked_apply(vectors, key_lag, key_lag, lower_table)
        return result + ridge_value * vectors

    solution = jnp.zeros_like(adjoint_rhs)
    residual_now = adjoint_rhs
    direction = adjoint_rhs
    norm_now = jnp.sum(residual_now * residual_now, axis=-1, keepdims=True)
    for iteration in range(ITERS):
        image = apply_gram(direction)
        alpha = norm_now / (jnp.sum(direction * image, axis=-1, keepdims=True) + EPSILON)
        solution = solution + alpha * direction
        residual_now = residual_now - alpha * image
        norm_next = jnp.sum(residual_now * residual_now, axis=-1, keepdims=True)
        direction = residual_now + (norm_next / (norm_now + EPSILON)) * direction
        norm_now = norm_next

    pair_blocks = outer_sums(solution, sav_blk)
    cross_blocks = outer_sums(sav_blk, out_blk)
    pair_after = jnp.flip(jnp.cumsum(jnp.flip(pair_blocks, 0), axis=0), 0) - pair_blocks
    cross_after = jnp.flip(jnp.cumsum(jnp.flip(cross_blocks, 0), axis=0), 0) - cross_blocks
    pair_base = pair_after - shift_up(pair_after, lag_blocks)
    cross_base = cross_after - shift_up(cross_after, lag_blocks)
    sym_base = pair_base + jnp.swapaxes(pair_base, 1, 2)

    sol_lead = shift_up(solution, lag_blocks)
    sav_lead = shift_up(sav_blk, lag_blocks)
    out_lead = shift_up(out_blk, lag_blocks)

    grad_k = -jnp.einsum("bid,bde->bie", key_blk, sym_base, precision=HIGHEST_PRECISION)
    grad_k = grad_k + jnp.einsum("bif,bef->bie", val_blk, cross_base, precision=HIGHEST_PRECISION)
    grad_k = grad_k - masked_apply(key_blk, sav_blk, solution, upper_table)
    grad_k = grad_k - masked_apply(key_blk, solution, sav_blk, upper_table)
    grad_k = grad_k + masked_apply(val_blk, out_blk, sav_blk, upper_table)
    grad_k = grad_k + masked_apply(key_blk, sav_lead, sol_lead, upper_table)
    grad_k = grad_k + masked_apply(key_blk, sol_lead, sav_lead, upper_table)
    grad_k = grad_k - masked_apply(val_blk, out_lead, sav_lead, upper_table)

    grad_v = jnp.einsum("bid,bdf->bif", key_blk, cross_base, precision=HIGHEST_PRECISION)
    grad_v = grad_v + masked_apply(key_blk, sav_blk, out_blk, upper_table)
    grad_v = grad_v - masked_apply(key_blk, sav_lead, out_lead, upper_table)

    return (solution.reshape(TOKENS, DH), grad_k.reshape(TOKENS, DH), grad_v.reshape(TOKENS, DH))


def reference(key_rows, values, d_layer, out_weight, saved_solutions, ridge_scale):
    d_heads = jnp.dot(d_layer, out_weight.T, preferred_element_type=jnp.float32).astype(jnp.bfloat16)

    def by_head(array):
        return array.astype(jnp.float32).reshape(TOKENS, HEADS, DH).transpose(1, 0, 2)

    grads = lax.map(one_head, (by_head(key_rows), by_head(values), by_head(saved_solutions),
                               by_head(d_heads), ridge_scale.astype(jnp.float32)))

    def by_token(array):
        return array.transpose(1, 0, 2).reshape(TOKENS, HEADS * DH).astype(jnp.float32)

    return by_token(grads[0]), by_token(grads[1]), by_token(grads[2])
```

```python
import jax
import jax.numpy as jnp
from jax import lax
from jax.experimental import pallas as pl
from jax.experimental.pallas import tpu as pltpu
from jax.sharding import PartitionSpec as P

DH = 128
ITERS = 8
EPSILON = 1e-06
BF = jnp.bfloat16
F32 = jnp.float32


def shift(block, axis, distance):
    devices = range(lax.axis_size(axis))
    route = [(i - distance, i) for i in devices if i - distance in devices]
    return lax.ppermute(block, axis, route)


def rotate(block, axis, distance):
    n = lax.axis_size(axis)
    return lax.ppermute(block, axis, [(i, (i + distance) % n) for i in range(n)])


def nn(left, right):
    return lax.dot_general(left, right, (((1,), (0,)), ((), ())), preferred_element_type=F32)


def nt(left, right):
    return lax.dot_general(left, right, (((1,), (1,)), ((), ())), preferred_element_type=F32)


def split(a):
    hi = a.astype(BF)
    return hi, (a - hi.astype(F32)).astype(BF)


def flip(a):
    return a.astype(F32).T.astype(BF)


def head(ref, h):
    return ref[:, h * DH : (h + 1) * DH]


def window_masked(scores):
    tok = scores.shape[1]
    key_ids = lax.broadcasted_iota(jnp.int32, (tok, tok), 0)
    tok_ids = lax.broadcasted_iota(jnp.int32, (tok, tok), 1)
    own = key_ids <= tok_ids
    return jnp.concatenate(
        [jnp.where(own, scores[:tok], 0.0), jnp.where(own, 0.0, scores[tok:])], axis=0
    )


def rhs_kernel(index, *refs):
    pieces, rest = refs[:-10], refs[-10:]
    w, key, val, key_lag, val_lag, state, sav, out, rhs, cross = rest
    n = len(pieces)
    width = pieces[0].shape[1]
    acc = None
    for j in range(n):
        col = lax.rem(index[0] + (n - j), n) * width
        part = nt(pieces[j][...], w[:, pl.ds(pl.multiple_of(col, width), width)])
        acc = part if acc is None else acc + part
    o_all = acc.astype(BF)
    out[...] = o_all
    for h in range(state.shape[0]):
        o = o_all[:, h * DH : (h + 1) * DH]
        v_cat = jnp.concatenate([head(val, h), head(val_lag, h)], axis=0)
        k_t = flip(jnp.concatenate([head(key, h), head(key_lag, h)], axis=0))
        s_hi, s_lo = split(window_masked(nt(v_cat, o)))
        st_hi, st_lo = split(state[h])
        rhs[h] = nn(k_t, s_hi) + nn(k_t, s_lo) + nt(st_hi, o) + nt(st_lo, o)
        x_hi, x_lo = split(head(sav, h).T)
        cross[h] = nn(x_hi, o) + nn(x_lo, o)


def cg_kernel(ridge, rhs, key, key_lag, gram, sav, sol, sol_bf, pair, r_s, p_s, y_s, rr_s, k2_s, kt_s, g_s):
    heads = rhs.shape[0]
    for h in range(heads):
        k_cat = jnp.concatenate([head(key, h), head(key_lag, h)], axis=0)
        k2_s[h] = jnp.concatenate([k_cat, k_cat], axis=1)
        kt_s[h] = flip(k_cat)
        g_hi, g_lo = split(gram[h])
        g_s[h] = jnp.concatenate([g_hi, g_hi, g_lo], axis=1)
        r = rhs[h]
        r_s[h] = r
        p_s[h] = r
        y_s[h] = jnp.zeros_like(r)
        rr_s[h] = jnp.sum(r * r, axis=0, keepdims=True)

    def step(_, carry):
        for h in range(heads):
            p = p_s[h]
            p_hi, p_lo = split(p)
            scores = nn(k2_s[h], jnp.concatenate([p_hi, p_lo], axis=0))
            s = window_masked(scores).astype(BF)
            image = nn(kt_s[h], s) + nn(g_s[h], jnp.concatenate([p_hi, p_lo, p_hi], axis=0))
            image = image + ridge[h] * p
            rr = rr_s[h]
            alpha = rr / (jnp.sum(p * image, axis=0, keepdims=True) + EPSILON)
            y_s[h] = y_s[h] + alpha * p
            r = r_s[h] - alpha * image
            r_s[h] = r
            nr = jnp.sum(r * r, axis=0, keepdims=True)
            p_s[h] = r + nr / (rr + EPSILON) * p
            rr_s[h] = nr
        return carry

    lax.fori_loop(0, ITERS, step, 0)
    for h in range(heads):
        y = y_s[h].T
        sol[:, h * DH : (h + 1) * DH] = y
        y_hi, y_lo = split(y)
        sol_bf[:, h * DH : (h + 1) * DH] = y_hi
        x_hi, x_lo = split(head(sav, h).T)
        pair[h] = (nn(x_hi, y_hi) + nn(x_lo, y_hi) + nn(x_hi, y_lo)).astype(BF)


def own_kernel(key, val, sol, sav, out, gk, gv):
    tok = key.shape[0]
    key_ids = lax.broadcasted_iota(jnp.int32, (tok, tok), 0)
    tok_ids = lax.broadcasted_iota(jnp.int32, (tok, tok), 1)
    later = tok_ids >= key_ids
    for h in range(key.shape[1] // DH):
        k, v, o = head(key, h), head(val, h), head(out, h)
        x_hi, x_lo = split(head(sav, h))
        y_hi, y_lo = split(-head(sol, h))
        a1 = nt(jnp.concatenate([k, k], axis=1), jnp.concatenate([x_hi, x_lo], axis=1))
        a2 = nt(jnp.concatenate([v, k], axis=1), jnp.concatenate([o, y_hi], axis=1)) + nt(k, y_lo)
        a1_hi, a1_lo = split(jnp.where(later, a1, 0.0))
        a2_hi, a2_lo = split(jnp.where(later, a2, 0.0))
        yo = jnp.concatenate([y_hi, o], axis=1)
        both = nn(a1_hi, yo) + nn(a1_lo, yo)
        g = both[:, :DH] + nn(a1_hi, y_lo) + nn(a2_hi, x_hi) + nn(a2_lo, x_hi) + nn(a2_hi, x_lo)
        gk[:, h * DH : (h + 1) * DH] = g
        gv[:, h * DH : (h + 1) * DH] = both[:, DH:]


def lead_kernel(key, val, sol, sav, out, pair, cross, gk_own, gv_own, gk, gv):
    tok = key.shape[0]
    key_ids = lax.broadcasted_iota(jnp.int32, (tok, tok), 0)
    tok_ids = lax.broadcasted_iota(jnp.int32, (tok, tok), 1)
    later = tok_ids < key_ids
    for h in range(key.shape[1] // DH):
        k, v, o, x, y = head(key, h), head(val, h), head(out, h), head(sav, h), -head(sol, h)
        vk = jnp.concatenate([v, k], axis=1)
        a1_hi, a1_lo = split(jnp.where(later, nt(k, x), 0.0))
        a2_hi, a2_lo = split(jnp.where(later, nt(vk, jnp.concatenate([o, y], axis=1)), 0.0))
        yo = jnp.concatenate([y, o], axis=1)
        c_hi, c_lo = split(cross[h])
        p_hi, p_lo = split(-pair[h])
        both = nn(a1_hi, yo) + nn(a1_lo, yo)
        both = both + nn(k, jnp.concatenate([p_hi, c_hi], axis=1)) + nn(k, jnp.concatenate([p_lo, c_lo], axis=1))
        g = both[:, :DH] + nn(a2_hi, x) + nn(a2_lo, x)
        g = g + nt(vk, jnp.concatenate([c_hi, p_hi], axis=1)) + nt(vk, jnp.concatenate([c_lo, p_lo], axis=1))
        at = slice(h * DH, (h + 1) * DH)
        gk[:, at] = gk_own[:, at] + g
        gv[:, at] = gv_own[:, at] + both[:, DH:]


def totals_kernel(key, val, gram, state):
    for h in range(gram.shape[0]):
        k = head(key, h)
        k_t = flip(k)
        both = nn(k_t, jnp.concatenate([k, head(val, h)], axis=1))
        gram[h] = both[:, :DH]
        state[h] = both[:, DH:]


def call(kernel, name, outs, flops, args, scalars=0, scratch=()):
    vmem = pl.BlockSpec(memory_space=pltpu.VMEM)
    smem = pl.BlockSpec(memory_space=pltpu.SMEM)
    return pl.pallas_call(
        kernel,
        name=name,
        out_shape=outs,
        in_specs=[smem] * scalars + [vmem] * (len(args) - scalars),
        out_specs=[vmem] * len(outs),
        scratch_shapes=list(scratch),
        cost_estimate=pl.CostEstimate(flops=flops, bytes_accessed=1 << 20, transcendentals=0),
        compiler_params=pltpu.CompilerParams(vmem_limit_bytes=40 << 20),
    )(*args)


def sum_over_mid(arrays, span, sign):
    total = None
    for d in range(1, span):
        arrived = [shift(a, "seq", sign * d).astype(F32) for a in arrays]
        total = arrived if total is None else [a + b for a, b in zip(total, arrived)]
    if total is None:
        total = [jnp.zeros(a.shape, F32) for a in arrays]
    return total


def body(key_rows, values, d_layer, out_weight, saved_solutions, ridge_scale):
    tok, cols = key_rows.shape
    heads = cols // DH
    span = lax.axis_size("seq") // 4
    n_head = lax.axis_size("head")
    sds = jax.ShapeDtypeStruct
    mats = sds((heads, DH, DH), F32)
    unit = 2 * tok * tok * DH * heads

    pieces = [d_layer] + [rotate(d_layer, "head", j) for j in range(1, n_head)]
    key_lag = shift(key_rows, "seq", span)
    val_lag = shift(values, "seq", span)
    sav_bf = saved_solutions.astype(BF)
    sav_lead = shift(sav_bf, "seq", -span)
    gram_own, state_own = call(totals_kernel, "totals", [mats, mats], unit, (key_rows, values))
    gram_mid, state_mid = sum_over_mid([gram_own, state_own], span, 1)

    index = lax.axis_index("head").reshape(1)
    out, rhs, cross = call(
        rhs_kernel,
        "rhs",
        [sds((tok, cols), BF), sds((heads, DH, tok), F32), mats],
        8 * unit,
        (index, *pieces, out_weight, key_rows, values, key_lag, val_lag, state_mid, saved_solutions),
        scalars=1,
    )
    out_lead = shift(out, "seq", -span)
    (cross_mid,) = sum_over_mid([cross], span, -1)
    vec = pltpu.VMEM((heads, DH, tok), F32)
    sol, sol_bf, pair = call(
        cg_kernel,
        "cg",
        [sds((tok, cols), F32), sds((tok, cols), BF), sds((heads, DH, DH), BF)],
        100 * unit,
        (ridge_scale, rhs, key_rows, key_lag, gram_mid, saved_solutions),
        scalars=1,
        scratch=[
            vec,
            vec,
            vec,
            pltpu.VMEM((heads, 1, tok), F32),
            pltpu.VMEM((heads, 2 * tok, 2 * DH), BF),
            pltpu.VMEM((heads, DH, 2 * tok), BF),
            pltpu.VMEM((heads, DH, 3 * DH), BF),
        ],
    )
    sol_lead = shift(sol_bf, "seq", -span)
    (pair_mid,) = sum_over_mid([pair], span, -1)
    flat = sds((tok, cols), F32)
    gk_own, gv_own = call(
        own_kernel, "own", [flat, flat], 10 * unit, (key_rows, values, sol, saved_solutions, out)
    )
    gk, gv = call(
        lead_kernel,
        "lead",
        [flat, flat],
        8 * unit,
        (key_rows, values, sol_lead, sav_lead, out_lead, pair_mid, cross_mid, gk_own, gv_own),
    )
    return sol, gk, gv


def solution(mesh):
    return jax.shard_map(
        body,
        mesh=mesh,
        in_specs=(
            P("seq", "head"),
            P("seq", "head"),
            P("seq", "head"),
            P("head", None),
            P("seq", "head"),
            P("head"),
        ),
        out_specs=(P("seq", "head"), P("seq", "head"), P("seq", "head")),
        check_vma=False,
    )
```

```python
import functools
import jax
import jax.numpy as jnp
from jax import lax
from jax.experimental import pallas as pl
from jax.experimental.pallas import tpu as pltpu
from jax.sharding import PartitionSpec as P

DH = 128
ITERS = 8
EPSILON = 1e-06
BF = jnp.bfloat16
F32 = jnp.float32

def nn(left, right):
    return lax.dot_general(left, right, (((1,), (0,)), ((), ())), preferred_element_type=F32)


def nt(left, right):
    return lax.dot_general(left, right, (((1,), (1,)), ((), ())), preferred_element_type=F32)


def split(a):
    hi = a.astype(BF)
    return hi, (a - hi.astype(F32)).astype(BF)


def flip(a):
    return a.astype(F32).T.astype(BF)


def head(ref, h):
    return ref[:, h * DH : (h + 1) * DH]


def window_masked(scores):
    tok = scores.shape[1]
    key_ids = lax.broadcasted_iota(jnp.int32, (tok, tok), 0)
    tok_ids = lax.broadcasted_iota(jnp.int32, (tok, tok), 1)
    own = key_ids <= tok_ids
    return jnp.concatenate(
        [jnp.where(own, scores[:tok], 0.0), jnp.where(own, 0.0, scores[tok:])], axis=0
    )


def rows_sum(ref, h):
    total = None
    for slot in range(ref.shape[0]):
        part = ref[slot, h].astype(F32)
        total = part if total is None else total + part
    return total


def own_kernel(key, val, sol, sav, out, gk, gv):
    tok = key.shape[0]
    key_ids = lax.broadcasted_iota(jnp.int32, (tok, tok), 0)
    tok_ids = lax.broadcasted_iota(jnp.int32, (tok, tok), 1)
    later = tok_ids >= key_ids
    for h in range(key.shape[1] // DH):
        k, v, o = head(key, h), head(val, h), head(out, h)
        x_hi, x_lo = split(head(sav, h))
        y_hi, y_lo = split(-head(sol, h))
        a1 = nt(jnp.concatenate([k, k], axis=1), jnp.concatenate([x_hi, x_lo], axis=1))
        a2 = nt(jnp.concatenate([v, k], axis=1), jnp.concatenate([o, y_hi], axis=1)) + nt(k, y_lo)
        a1_hi, a1_lo = split(jnp.where(later, a1, 0.0))
        a2_hi, a2_lo = split(jnp.where(later, a2, 0.0))
        yo = jnp.concatenate([y_hi, o], axis=1)
        both = nn(a1_hi, yo) + nn(a1_lo, yo)
        g = both[:, :DH] + nn(a1_hi, y_lo) + nn(a2_hi, x_hi) + nn(a2_lo, x_hi) + nn(a2_hi, x_lo)
        gk[:, h * DH : (h + 1) * DH] = g
        gv[:, h * DH : (h + 1) * DH] = both[:, DH:]


def lead_kernel(key, val, sol, sav, out, pair, cross, gk_own, gv_own, gk, gv):
    tok = key.shape[0]
    key_ids = lax.broadcasted_iota(jnp.int32, (tok, tok), 0)
    tok_ids = lax.broadcasted_iota(jnp.int32, (tok, tok), 1)
    later = tok_ids < key_ids
    for h in range(key.shape[1] // DH):
        k, v, o, x, y = head(key, h), head(val, h), head(out, h), head(sav, h), -head(sol, h)
        vk = jnp.concatenate([v, k], axis=1)
        a1_hi, a1_lo = split(jnp.where(later, nt(k, x), 0.0))
        a2_hi, a2_lo = split(jnp.where(later, nt(vk, jnp.concatenate([o, y], axis=1)), 0.0))
        yo = jnp.concatenate([y, o], axis=1)
        c_hi, c_lo = split(rows_sum(cross, h))
        p_hi, p_lo = split(-rows_sum(pair, h))
        both = nn(a1_hi, yo) + nn(a1_lo, yo)
        both = both + nn(k, jnp.concatenate([p_hi, c_hi], axis=1)) + nn(k, jnp.concatenate([p_lo, c_lo], axis=1))
        g = both[:, :DH] + nn(a2_hi, x) + nn(a2_lo, x)
        g = g + nt(vk, jnp.concatenate([c_hi, p_hi], axis=1)) + nt(vk, jnp.concatenate([c_lo, p_lo], axis=1))
        at = slice(h * DH, (h + 1) * DH)
        gk[:, at] = gk_own[:, at] + g
        gv[:, at] = gv_own[:, at] + both[:, DH:]


def mega(span, n_seq, n_head, ridge, key, val, d_own, w_hbm, sav_hbm, sol, gk, gv,
         w, sav, sav_bf, out, sol_bf, gram, state, cross, pair,
         d_in, key_lag, val_lag, sav_lead, out_lead, sol_lead, gram_in, state_in, cross_in, pair_in,
         r_s, p_s, y_s, rr_s, k2_s, kt_s, g_s, local_sem, send_sem, recv_sem):
    s = lax.axis_index("seq")
    me = lax.axis_index("head")
    heads = gram.shape[0]
    tok = key.shape[0]
    w_copy = pltpu.make_async_copy(w_hbm, w, local_sem.at[0])
    x_copy = pltpu.make_async_copy(sav_hbm, sav, local_sem.at[1])
    w_copy.start()
    x_copy.start()

    offsets = [d for m in range(1, span + 1) for d in (m, -m)]

    def exists(d):
        return s + d < n_seq if d > 0 else s + d >= 0

    barrier = pltpu.get_barrier_semaphore()
    for j in range(1, n_head):
        pl.semaphore_signal(
            barrier, inc=1, device_id={"head": lax.rem(me + j, n_head)}, device_id_type=pl.DeviceIdType.MESH
        )
    for d in offsets:
        @pl.when(exists(d))
        def _():
            pl.semaphore_signal(barrier, inc=1, device_id={"seq": s + d}, device_id_type=pl.DeviceIdType.MESH)
    pl.semaphore_wait(
        barrier, n_head - 1 + jnp.minimum(s, span) + jnp.minimum(n_seq - 1 - s, span)
    )

    counter = [0]
    sends = []

    class Hop:
        def __init__(self, source, target, d):
            self.d = d
            self.copy = pltpu.make_async_remote_copy(
                src_ref=source,
                dst_ref=target,
                send_sem=send_sem.at[counter[0]],
                recv_sem=recv_sem.at[counter[0]],
                device_id={"seq": s + d},
                device_id_type=pl.DeviceIdType.MESH,
            )
            counter[0] += 1
            sends.append(self)

            @pl.when(jnp.logical_not(exists(-d)))
            def _():
                target[...] = jnp.zeros(target.shape, target.dtype)

        def start(self):
            pl.when(exists(self.d))(self.copy.start)
            return self

        def arrive(self):
            pl.when(exists(-self.d))(self.copy.wait_recv)

        def finish(self):
            pl.when(exists(self.d))(self.copy.wait_send)

    def mids(source, target, sign):
        return [Hop(source, target.at[m - 1], sign * m).start() for m in range(1, span)]

    key_hop = Hop(key, key_lag, span).start()
    d_copies = []
    for j in range(1, n_head):
        copy = pltpu.make_async_remote_copy(
            src_ref=d_own,
            dst_ref=d_in.at[j - 1],
            send_sem=send_sem.at[counter[0]],
            recv_sem=recv_sem.at[counter[0]],
            device_id={"head": lax.rem(me + j, n_head)},
            device_id_type=pl.DeviceIdType.MESH,
        )
        counter[0] += 1
        copy.start()
        d_copies.append(copy)
    val_hop = Hop(val, val_lag, span).start()

    for h in range(heads):
        k = head(key, h)
        both = nn(flip(k), jnp.concatenate([k, head(val, h)], axis=1)).astype(BF)
        gram[h] = both[:, :DH]
        state[h] = both[:, DH:]
    state_hops = mids(state, state_in, 1)
    gram_hops = mids(gram, gram_in, 1)
    x_copy.wait()
    sav_bf[...] = sav[...].astype(BF)
    sav_hop = Hop(sav_bf, sav_lead, -span).start()

    w_copy.wait()
    width = d_own.shape[1]
    acc = None
    for j in range(n_head):
        if j:
            d_copies[j - 1].wait_recv()
        piece = d_own[...] if j == 0 else d_in[j - 1]
        col = lax.rem(me + (n_head - j), n_head) * width
        part = nt(piece, w[:, pl.ds(pl.multiple_of(col, width), width)])
        acc = part if acc is None else acc + part
    out[...] = acc.astype(BF)
    out_hop = Hop(out, out_lead, -span).start()
    for h in range(heads):
        x_hi, x_lo = split(head(sav, h).T)
        o = head(out, h)
        cross[h] = (nn(x_hi, o) + nn(x_lo, o)).astype(BF)
    cross_hops = mids(cross, cross_in, -1)

    key_hop.arrive()
    for h in range(heads):
        k_cat = jnp.concatenate([head(key, h), head(key_lag, h)], axis=0)
        k2_s[h] = jnp.concatenate([k_cat, k_cat], axis=1)
        kt_s[h] = flip(k_cat)
    val_hop.arrive()
    for hop in state_hops + gram_hops:
        hop.arrive()
    for h in range(heads):
        o = head(out, h)
        v_cat = jnp.concatenate([head(val, h), head(val_lag, h)], axis=0)
        s_hi, s_lo = split(window_masked(nt(v_cat, o)))
        st_hi, st_lo = split(rows_sum(state_in, h))
        r = nn(kt_s[h], s_hi) + nn(kt_s[h], s_lo) + nt(st_hi, o) + nt(st_lo, o)
        g_hi, g_lo = split(rows_sum(gram_in, h))
        g_s[h] = jnp.concatenate([g_hi, g_hi, g_lo], axis=1)
        r_s[h] = r
        p_s[h] = r
        y_s[h] = jnp.zeros_like(r)
        rr_s[h] = jnp.sum(r * r, axis=0, keepdims=True)

    def step(_, carry):
        for h in range(heads):
            p = p_s[h]
            p_hi, p_lo = split(p)
            scores = nn(k2_s[h], jnp.concatenate([p_hi, p_lo], axis=0))
            masked = window_masked(scores).astype(BF)
            image = nn(kt_s[h], masked) + nn(g_s[h], jnp.concatenate([p_hi, p_lo, p_hi], axis=0))
            image = image + ridge[h] * p
            rr = rr_s[h]
            alpha = rr / (jnp.sum(p * image, axis=0, keepdims=True) + EPSILON)
            y_s[h] = y_s[h] + alpha * p
            r = r_s[h] - alpha * image
            r_s[h] = r
            nr = jnp.sum(r * r, axis=0, keepdims=True)
            p_s[h] = r + nr / (rr + EPSILON) * p
            rr_s[h] = nr
        return carry

    lax.fori_loop(0, ITERS, step, 0)
    for h in range(heads):
        y = y_s[h].T
        sol[:, h * DH : (h + 1) * DH] = y
        sol_bf[:, h * DH : (h + 1) * DH] = y.astype(BF)
    sol_hop = Hop(sol_bf, sol_lead, -span).start()
    for h in range(heads):
        y_hi, y_lo = split(head(sol, h))
        x_hi, x_lo = split(head(sav, h).T)
        pair[h] = (nn(x_hi, y_hi) + nn(x_lo, y_hi) + nn(x_hi, y_lo)).astype(BF)
    pair_hops = mids(pair, pair_in, -1)

    own_kernel(key, val, sol, sav, out, gk, gv)
    for hop in [sav_hop, out_hop] + cross_hops + [sol_hop] + pair_hops:
        hop.arrive()
    lead_kernel(key, val, sol_lead, sav_lead, out_lead, pair_in, cross_in, gk, gv, gk, gv)
    for copy in d_copies:
        copy.wait_send()
    for hop in sends:
        hop.finish()


def body(key_rows, values, d_layer, out_weight, saved_solutions, ridge_scale):
    tok, cols = key_rows.shape
    heads = cols // DH
    n_seq, n_head = lax.axis_size("seq"), lax.axis_size("head")
    span = n_seq // 4
    slots = max(span - 1, 1)
    copies = n_head - 1 + 5 + 4 * (span - 1)
    vmem = pl.BlockSpec(memory_space=pltpu.VMEM)
    smem = pl.BlockSpec(memory_space=pltpu.SMEM)
    hbm = pl.BlockSpec(memory_space=pl.ANY)
    flat = jax.ShapeDtypeStruct((tok, cols), F32)
    half = pltpu.VMEM((tok, cols), BF)
    mats = pltpu.VMEM((heads, DH, DH), BF)
    mats_in = pltpu.VMEM((slots, heads, DH, DH), BF)
    vec = pltpu.VMEM((heads, DH, tok), F32)
    return pl.pallas_call(
        functools.partial(mega, span, n_seq, n_head),
        name="layer",
        out_shape=[flat, flat, flat],
        in_specs=[smem, vmem, vmem, vmem, hbm, hbm],
        out_specs=[vmem, vmem, vmem],
        scratch_shapes=[
            pltpu.VMEM(out_weight.shape, BF), pltpu.VMEM((tok, cols), F32), half, half, half,
            mats, mats, mats, mats,
            pltpu.VMEM((n_head - 1,) + d_layer.shape, BF), half, half, half, half, half,
            mats_in, mats_in, mats_in, mats_in,
            vec, vec, vec,
            pltpu.VMEM((heads, 1, tok), F32),
            pltpu.VMEM((heads, 2 * tok, 2 * DH), BF),
            pltpu.VMEM((heads, DH, 2 * tok), BF),
            pltpu.VMEM((heads, DH, 3 * DH), BF),
            pltpu.SemaphoreType.DMA((2,)),
            pltpu.SemaphoreType.DMA((copies,)),
            pltpu.SemaphoreType.DMA((copies,)),
        ],
        compiler_params=pltpu.CompilerParams(
            collective_id=0, has_side_effects=True, vmem_limit_bytes=40 << 20
        ),
    )(ridge_scale, key_rows, values, d_layer, out_weight, saved_solutions)


def solution(mesh):
    return jax.shard_map(
        body,
        mesh=mesh,
        in_specs=(
            P("seq", "head"),
            P("seq", "head"),
            P("seq", "head"),
            P("head", None),
            P("seq", "head"),
            P("head"),
        ),
        out_specs=(P("seq", "head"), P("seq", "head"), P("seq", "head")),
        check_vma=False,
    )
```

```python
import functools
import jax
import jax.numpy as jnp
from jax import lax
from jax.experimental import pallas as pl
from jax.experimental.pallas import tpu as pltpu
from jax.sharding import PartitionSpec as P

DH = 128
ITERS = 8
EPSILON = 1e-06
BF = jnp.bfloat16
F32 = jnp.float32

def nn(left, right):
    return lax.dot_general(left, right, (((1,), (0,)), ((), ())), preferred_element_type=F32)


def nt(left, right):
    return lax.dot_general(left, right, (((1,), (1,)), ((), ())), preferred_element_type=F32)


def split(a):
    hi = a.astype(BF)
    return hi, (a - hi.astype(F32)).astype(BF)


def flip(a):
    return a.astype(F32).T.astype(BF)


def head(ref, h):
    return ref[:, h * DH : (h + 1) * DH]


def window_masked(scores):
    tok = scores.shape[1]
    key_ids = lax.broadcasted_iota(jnp.int32, (tok, tok), 0)
    tok_ids = lax.broadcasted_iota(jnp.int32, (tok, tok), 1)
    own = key_ids <= tok_ids
    return jnp.concatenate(
        [jnp.where(own, scores[:tok], 0.0), jnp.where(own, 0.0, scores[tok:])], axis=0
    )


def rows_sum(ref, h):
    total = None
    for slot in range(ref.shape[0]):
        part = ref[slot, h].astype(F32)
        total = part if total is None else total + part
    return total


def own_kernel(key, val, sol, sav, out, gk, gv):
    tok = key.shape[0]
    key_ids = lax.broadcasted_iota(jnp.int32, (tok, tok), 0)
    tok_ids = lax.broadcasted_iota(jnp.int32, (tok, tok), 1)
    later = tok_ids >= key_ids
    for h in range(key.shape[1] // DH):
        k, v, o = head(key, h), head(val, h), head(out, h)
        x_hi, x_lo = split(head(sav, h))
        y_hi, y_lo = split(-head(sol, h))
        a1 = nt(jnp.concatenate([k, k], axis=1), jnp.concatenate([x_hi, x_lo], axis=1))
        a2 = nt(jnp.concatenate([v, k], axis=1), jnp.concatenate([o, y_hi], axis=1)) + nt(k, y_lo)
        a1_hi, a1_lo = split(jnp.where(later, a1, 0.0))
        a2_hi, a2_lo = split(jnp.where(later, a2, 0.0))
        yo = jnp.concatenate([y_hi, o], axis=1)
        both = nn(a1_hi, yo) + nn(a1_lo, yo)
        g = both[:, :DH] + nn(a1_hi, y_lo) + nn(a2_hi, x_hi) + nn(a2_lo, x_hi) + nn(a2_hi, x_lo)
        gk[:, h * DH : (h + 1) * DH] = g
        gv[:, h * DH : (h + 1) * DH] = both[:, DH:]


def lead_kernel(key, val, sol, sav, out, pair, cross, gk_own, gv_own, gk, gv):
    tok = key.shape[0]
    key_ids = lax.broadcasted_iota(jnp.int32, (tok, tok), 0)
    tok_ids = lax.broadcasted_iota(jnp.int32, (tok, tok), 1)
    later = tok_ids < key_ids
    for h in range(key.shape[1] // DH):
        k, v, o, x, y = head(key, h), head(val, h), head(out, h), head(sav, h), -head(sol, h)
        vk = jnp.concatenate([v, k], axis=1)
        a1_hi, a1_lo = split(jnp.where(later, nt(k, x), 0.0))
        a2_hi, a2_lo = split(jnp.where(later, nt(vk, jnp.concatenate([o, y], axis=1)), 0.0))
        yo = jnp.concatenate([y, o], axis=1)
        c_hi, c_lo = split(rows_sum(cross, h))
        p_hi, p_lo = split(-rows_sum(pair, h))
        both = nn(a1_hi, yo) + nn(a1_lo, yo)
        both = both + nn(k, jnp.concatenate([p_hi, c_hi], axis=1)) + nn(k, jnp.concatenate([p_lo, c_lo], axis=1))
        g = both[:, :DH] + nn(a2_hi, x) + nn(a2_lo, x)
        g = g + nt(vk, jnp.concatenate([c_hi, p_hi], axis=1)) + nt(vk, jnp.concatenate([c_lo, p_lo], axis=1))
        at = slice(h * DH, (h + 1) * DH)
        gk[:, at] = gk_own[:, at] + g
        gv[:, at] = gv_own[:, at] + both[:, DH:]


def mega(span, n_seq, n_head, ridge, key_hbm, val_hbm, d_hbm, w_hbm, sav_hbm, sol, gk, gv,
         key, val, d_own, w, sav, sav_bf, out, sol_bf, gram, state, cross, pair,
         d_in, key_lag, val_lag, sav_lead, out_lead, sol_lead, gram_in, state_in, cross_in, pair_in,
         r_s, p_s, y_s, rr_s, k2_s, kt_s, g_s, local_sem, send_sem, recv_sem):
    s = lax.axis_index("seq")
    me = lax.axis_index("head")
    heads = gram.shape[0]
    tok = key.shape[0]
    w_copy = pltpu.make_async_copy(w_hbm, w, local_sem.at[0])
    x_copy = pltpu.make_async_copy(sav_hbm, sav, local_sem.at[1])
    inputs = [
        pltpu.make_async_copy(source, target, local_sem.at[2 + number])
        for number, (source, target) in enumerate([(key_hbm, key), (d_hbm, d_own), (val_hbm, val)])
    ]
    for copy in inputs:
        copy.start()
    w_copy.start()
    x_copy.start()

    offsets = [d for m in range(1, span + 1) for d in (m, -m)]

    def exists(d):
        return s + d < n_seq if d > 0 else s + d >= 0

    barrier = pltpu.get_barrier_semaphore()
    for j in range(1, n_head):
        pl.semaphore_signal(
            barrier, inc=1, device_id={"head": lax.rem(me + j, n_head)}, device_id_type=pl.DeviceIdType.MESH
        )
    for d in offsets:
        @pl.when(exists(d))
        def _():
            pl.semaphore_signal(barrier, inc=1, device_id={"seq": s + d}, device_id_type=pl.DeviceIdType.MESH)
    pl.semaphore_wait(
        barrier, n_head - 1 + jnp.minimum(s, span) + jnp.minimum(n_seq - 1 - s, span)
    )

    counter = [0]
    sends = []

    class Hop:
        def __init__(self, source, target, d):
            self.d = d
            self.copy = pltpu.make_async_remote_copy(
                src_ref=source,
                dst_ref=target,
                send_sem=send_sem.at[counter[0]],
                recv_sem=recv_sem.at[counter[0]],
                device_id={"seq": s + d},
                device_id_type=pl.DeviceIdType.MESH,
            )
            counter[0] += 1
            sends.append(self)

            @pl.when(jnp.logical_not(exists(-d)))
            def _():
                target[...] = jnp.zeros(target.shape, target.dtype)

        def start(self):
            pl.when(exists(self.d))(self.copy.start)
            return self

        def arrive(self):
            pl.when(exists(-self.d))(self.copy.wait_recv)

        def finish(self):
            pl.when(exists(self.d))(self.copy.wait_send)

    def mids(source, target, sign):
        return [Hop(source, target.at[m - 1], sign * m).start() for m in range(1, span)]

    for copy in inputs:
        copy.wait()
    key_hop = Hop(key, key_lag, span).start()
    d_copies = []
    for j in range(1, n_head):
        copy = pltpu.make_async_remote_copy(
            src_ref=d_own,
            dst_ref=d_in.at[j - 1],
            send_sem=send_sem.at[counter[0]],
            recv_sem=recv_sem.at[counter[0]],
            device_id={"head": lax.rem(me + j, n_head)},
            device_id_type=pl.DeviceIdType.MESH,
        )
        counter[0] += 1
        copy.start()
        d_copies.append(copy)
    val_hop = Hop(val, val_lag, span).start()

    for h in range(heads):
        k = head(key, h)
        both = nn(flip(k), jnp.concatenate([k, head(val, h)], axis=1)).astype(BF)
        gram[h] = both[:, :DH]
        state[h] = both[:, DH:]
    state_hops = mids(state, state_in, 1)
    gram_hops = mids(gram, gram_in, 1)
    x_copy.wait()
    sav_bf[...] = sav[...].astype(BF)
    sav_hop = Hop(sav_bf, sav_lead, -span).start()

    w_copy.wait()
    width = d_own.shape[1]
    acc = None
    for j in range(n_head):
        if j:
            d_copies[j - 1].wait_recv()
        piece = d_own[...] if j == 0 else d_in[j - 1]
        col = lax.rem(me + (n_head - j), n_head) * width
        part = nt(piece, w[:, pl.ds(pl.multiple_of(col, width), width)])
        acc = part if acc is None else acc + part
    out[...] = acc.astype(BF)
    out_hop = Hop(out, out_lead, -span).start()
    for h in range(heads):
        x_hi, x_lo = split(head(sav, h).T)
        o = head(out, h)
        cross[h] = (nn(x_hi, o) + nn(x_lo, o)).astype(BF)
    cross_hops = mids(cross, cross_in, -1)

    key_hop.arrive()
    for h in range(heads):
        k_cat = jnp.concatenate([head(key, h), head(key_lag, h)], axis=0)
        k2_s[h] = jnp.concatenate([k_cat, k_cat], axis=1)
        kt_s[h] = flip(k_cat)
    val_hop.arrive()
    for hop in state_hops + gram_hops:
        hop.arrive()
    for h in range(heads):
        o = head(out, h)
        v_cat = jnp.concatenate([head(val, h), head(val_lag, h)], axis=0)
        s_hi, s_lo = split(window_masked(nt(v_cat, o)))
        st_hi, st_lo = split(rows_sum(state_in, h))
        r = nn(kt_s[h], s_hi) + nn(kt_s[h], s_lo) + nt(st_hi, o) + nt(st_lo, o)
        g_hi, g_lo = split(rows_sum(gram_in, h))
        g_s[h] = jnp.concatenate([g_hi, g_hi, g_lo], axis=1)
        r_s[h] = r
        p_s[h] = r
        y_s[h] = jnp.zeros_like(r)
        rr_s[h] = jnp.sum(r * r, axis=0, keepdims=True)

    def step(_, carry):
        for h in range(heads):
            p = p_s[h]
            p_hi, p_lo = split(p)
            scores = nn(k2_s[h], jnp.concatenate([p_hi, p_lo], axis=0))
            masked = window_masked(scores).astype(BF)
            image = nn(kt_s[h], masked) + nn(g_s[h], jnp.concatenate([p_hi, p_lo, p_hi], axis=0))
            image = image + ridge[h] * p
            rr = rr_s[h]
            alpha = rr / (jnp.sum(p * image, axis=0, keepdims=True) + EPSILON)
            y_s[h] = y_s[h] + alpha * p
            r = r_s[h] - alpha * image
            r_s[h] = r
            nr = jnp.sum(r * r, axis=0, keepdims=True)
            p_s[h] = r + nr / (rr + EPSILON) * p
            rr_s[h] = nr
        return carry

    lax.fori_loop(0, ITERS, step, 0)
    for h in range(heads):
        y = y_s[h].T
        sol[:, h * DH : (h + 1) * DH] = y
        sol_bf[:, h * DH : (h + 1) * DH] = y.astype(BF)
    sol_hop = Hop(sol_bf, sol_lead, -span).start()
    for h in range(heads):
        y_hi, y_lo = split(head(sol, h))
        x_hi, x_lo = split(head(sav, h).T)
        pair[h] = (nn(x_hi, y_hi) + nn(x_lo, y_hi) + nn(x_hi, y_lo)).astype(BF)
    pair_hops = mids(pair, pair_in, -1)

    own_kernel(key, val, sol, sav, out, gk, gv)
    for hop in [sav_hop, out_hop] + cross_hops + [sol_hop] + pair_hops:
        hop.arrive()
    lead_kernel(key, val, sol_lead, sav_lead, out_lead, pair_in, cross_in, gk, gv, gk, gv)
    for copy in d_copies:
        copy.wait_send()
    for hop in sends:
        hop.finish()


def body(key_rows, values, d_layer, out_weight, saved_solutions, ridge_scale):
    tok, cols = key_rows.shape
    heads = cols // DH
    n_seq, n_head = lax.axis_size("seq"), lax.axis_size("head")
    span = n_seq // 4
    slots = max(span - 1, 1)
    copies = n_head - 1 + 5 + 4 * (span - 1)
    vmem = pl.BlockSpec(memory_space=pltpu.VMEM)
    smem = pl.BlockSpec(memory_space=pltpu.SMEM)
    hbm = pl.BlockSpec(memory_space=pltpu.HBM)
    flat = jax.ShapeDtypeStruct((tok, cols), F32)
    half = pltpu.VMEM((tok, cols), BF)
    mats = pltpu.VMEM((heads, DH, DH), BF)
    mats_in = pltpu.VMEM((slots, heads, DH, DH), BF)
    vec = pltpu.VMEM((heads, DH, tok), F32)
    return pl.pallas_call(
        functools.partial(mega, span, n_seq, n_head),
        name="layer",
        out_shape=[flat, flat, flat],
        in_specs=[smem, hbm, hbm, hbm, hbm, hbm],
        out_specs=[vmem, vmem, vmem],
        scratch_shapes=[
            half, half, pltpu.VMEM(d_layer.shape, BF),
            pltpu.VMEM(out_weight.shape, BF), pltpu.VMEM((tok, cols), F32), half, half, half,
            mats, mats, mats, mats,
            pltpu.VMEM((n_head - 1,) + d_layer.shape, BF), half, half, half, half, half,
            mats_in, mats_in, mats_in, mats_in,
            vec, vec, vec,
            pltpu.VMEM((heads, 1, tok), F32),
            pltpu.VMEM((heads, 2 * tok, 2 * DH), BF),
            pltpu.VMEM((heads, DH, 2 * tok), BF),
            pltpu.VMEM((heads, DH, 3 * DH), BF),
            pltpu.SemaphoreType.DMA((5,)),
            pltpu.SemaphoreType.DMA((copies,)),
            pltpu.SemaphoreType.DMA((copies,)),
        ],
        compiler_params=pltpu.CompilerParams(
            collective_id=0, has_side_effects=True, vmem_limit_bytes=67043328
        ),
    )(ridge_scale, key_rows, values, d_layer, out_weight, saved_solutions)


def solution(mesh):
    return jax.shard_map(
        body,
        mesh=mesh,
        in_specs=(
            P("seq", "head"),
            P("seq", "head"),
            P("seq", "head"),
            P("head", None),
            P("seq", "head"),
            P("head"),
        ),
        out_specs=(P("seq", "head"), P("seq", "head"), P("seq", "head")),
        check_vma=False,
    )
```
